32 devices in a mesh: seq: 8 (over z, x), tensor: 4 (over y, core).
Axes of the slice: x: 2, y: 2, z: 4, core: 2. Of those that a mesh axis runs over, the one named last changes fastest.
Arguments:
- tokens: bfloat16 [4096, 2048], P('seq', 'tensor'), may hold values from -12 to 12
- attn_gain: float32 [2048], replicated, may hold values from 0.1 to 1.9
- w_query: bfloat16 [2048, 2048], P('seq', 'tensor'), as said below
- w_key: bfloat16 [2048, 512], P('seq', 'tensor'), as said below
- w_value: bfloat16 [2048, 512], P('seq', 'tensor'), may hold values from -0.125 to 0.125
- w_out: bfloat16 [2048, 2048], P('tensor', 'seq'), may hold values from -0.125 to 0.125
- mlp_gain: float32 [2048], replicated, may hold values from 0.1 to 1.9
- w_gate: bfloat16 [2048, 5632], P('seq', 'tensor'), may hold values from -0.125 to 0.125
- w_up: bfloat16 [2048, 5632], P('seq', 'tensor'), may hold values from -0.125 to 0.125
- w_down: bfloat16 [5632, 2048], P('tensor', 'seq'), may hold values from -0.078125 to 0.078125
Outputs:
- layer_out: bfloat16 [4096, 2048], P('seq', 'tensor')
The draws below stay inside these ranges and needn't reach their ends.
Inputs may be any that keep to these rules, and one draw needn't show every extreme that they name: `w_query`: entries are of order 2048 to the power -1/2. `w_key`: entries are of order 2048 to the power -1/2.
All inputs are finite; a program needn't handle non-finite values.
Results may differ from the reference program's by a relative error of at most 0.013.
Values may be sent and summed in bfloat16 or wider, within the bound.
A program may use at most 128 MiB of HBM per device.

```python
import jax
import jax.numpy as jnp
from jax import lax

D = 2048
HEADS = 16
KV_HEADS = 4
HEAD_DIM = 128
FF = 5632
WINDOW = 1024
TOK_DEV = 512
TOKENS = 4096


def draw_tokens(key, part):
    noise = jax.random.normal(jax.random.fold_in(key, 31), (TOKENS, D), jnp.float32)
    return jnp.clip(noise, -12.0, 12.0).astype(jnp.bfloat16)


def draw_w_query(key, part):
    base = jax.random.normal(jax.random.fold_in(key, 21), (D, HEADS * HEAD_DIM), jnp.float32) / jnp.sqrt(1.0 * D)
    bound = 9.0 / jnp.sqrt(1.0 * D)
    return jnp.clip(base, -bound, bound).astype(jnp.bfloat16)


def draw_w_key(key, part):
    base = jax.random.normal(jax.random.fold_in(key, 22), (D, KV_HEADS * HEAD_DIM), jnp.float32) / jnp.sqrt(1.0 * D)
    bound = 9.0 / jnp.sqrt(1.0 * D)
    return jnp.clip(base, -bound, bound).astype(jnp.bfloat16)


def level_of(rng, extent, pieces, smallest, largest):
    level = 1.0
    for axis_at, shards_of in pieces:
        draws = jax.random.uniform(jax.random.fold_in(jax.random.fold_in(rng, 6), axis_at), (shards_of,), jnp.float32, smallest / len(pieces), largest / len(pieces))
        level = level * jnp.repeat(jnp.exp(draws), extent[axis_at] // shards_of).reshape((-1,) + (1,) * (len(extent) - 1 - axis_at))
    return level


def scatter_about(rng, shape, width, most, shards=(), kind=jnp.bfloat16):
    result = width * jax.random.normal(rng, shape, jnp.float32)
    if shards:
        result = result * level_of(rng, shape, shards, -0.22, 0.18)
    return jnp.clip(result, -most, most).astype(kind)


def setup_inputs(seed: int = 0) -> dict:
    arg_keys = jax.random.split(jax.random.key(seed), 11)
    return {
        "tokens": draw_tokens(jax.random.fold_in(arg_keys[10], 71), 0),
        "attn_gain": jnp.clip(1.0 + 0.18 * jax.random.normal(arg_keys[1], (D,), jnp.float32), 0.1, 1.9),
        "w_query": draw_w_query(jax.random.fold_in(arg_keys[10], 71), 0),
        "w_key": draw_w_key(jax.random.fold_in(arg_keys[10], 71), 0),
        "w_value": scatter_about(arg_keys[4], (D, KV_HEADS * HEAD_DIM), D ** -0.5, 0.125, ((0, 8), (1, 4))),
        "w_out": scatter_about(arg_keys[5], (HEADS * HEAD_DIM, D), (HEADS * HEAD_DIM) ** -0.5, 0.125, ((0, 4), (1, 8))),
        "mlp_gain": jnp.clip(1.0 + 0.18 * jax.random.normal(arg_keys[6], (D,), jnp.float32), 0.1, 1.9),
        "w_gate": scatter_about(arg_keys[7], (D, FF), D ** -0.5, 0.125, ((0, 8), (1, 4))),
        "w_up": scatter_about(arg_keys[8], (D, FF), D ** -0.5, 0.125, ((0, 8), (1, 4))),
        "w_down": scatter_about(arg_keys[9], (FF, D), FF ** -0.5, 0.078125, ((0, 4), (1, 8))),
    }


def scaled_rows(values, gain):
    values = values.astype(jnp.float32)
    mean_square = lax.optimization_barrier(jnp.mean(values * values, axis=1, keepdims=True))
    return (values * lax.rsqrt(mean_square + 1e-06) * gain.astype(jnp.float32)).astype(jnp.bfloat16)

def reference(tokens, attn_gain, w_query, w_key, w_value, w_out, mlp_gain, w_gate, w_up, w_down):
    normed = scaled_rows(tokens, attn_gain)
    queries = jnp.dot(normed, w_query, preferred_element_type=jnp.float32).astype(jnp.bfloat16)
    keys = jnp.dot(normed, w_key, preferred_element_type=jnp.float32).astype(jnp.bfloat16)
    values = jnp.dot(normed, w_value, preferred_element_type=jnp.float32).astype(jnp.bfloat16)
    group = HEADS // KV_HEADS
    block = min(512, TOK_DEV)
    count = TOKENS // block
    span = WINDOW + block
    scale = HEAD_DIM ** (-0.5)
    grouped = queries.reshape(TOKENS, KV_HEADS, group, HEAD_DIM)
    padding = jnp.zeros((WINDOW, KV_HEADS * HEAD_DIM), keys.dtype)
    keys_padded = jnp.concatenate([padding, keys], axis=0)
    values_padded = jnp.concatenate([padding, values], axis=0)

    def one_block(index):
        start = (index * block).astype(jnp.int32)
        query_block = lax.dynamic_slice_in_dim(grouped, start, block, 0)
        key_block = lax.dynamic_slice_in_dim(keys_padded, start, span, 0).reshape(span, KV_HEADS, HEAD_DIM)
        value_block = lax.dynamic_slice_in_dim(values_padded, start, span, 0).reshape(span, KV_HEADS, HEAD_DIM)
        scores = jnp.einsum('qkgd,ckd->kgqc', query_block.astype(jnp.float32), key_block.astype(jnp.float32)) * scale
        query_pos = lax.broadcasted_iota(jnp.int32, (block, span), 0)
        key_pos = lax.broadcasted_iota(jnp.int32, (block, span), 1)
        distance = query_pos + WINDOW - key_pos
        allowed = (distance >= 0) & (distance < WINDOW) & (key_pos + start - WINDOW >= 0)
        scores = jnp.where(allowed[None, None], scores, -1e+30)
        highest = lax.optimization_barrier(jnp.max(scores, axis=3, keepdims=True))
        raised = jnp.exp(scores - highest)
        weights = (raised / lax.optimization_barrier(jnp.sum(raised, axis=3, keepdims=True))).astype(jnp.bfloat16)
        mixed = jnp.einsum('kgqc,ckd->qkgd', weights.astype(jnp.float32), value_block.astype(jnp.float32))
        return mixed.astype(jnp.bfloat16).reshape(block, HEADS * HEAD_DIM)
    attended = lax.map(one_block, jnp.arange(count, dtype=jnp.int32)).reshape(TOKENS, HEADS * HEAD_DIM)
    group_width = group * HEAD_DIM
    attn_sum = jnp.zeros((TOKENS, D), jnp.float32)
    for head_group in range(KV_HEADS):
        lower = head_group * group_width
        term = jnp.dot(attended[:, lower:lower + group_width], w_out[lower:lower + group_width], preferred_element_type=jnp.float32)
        term = lax.optimization_barrier(term.astype(jnp.bfloat16))
        attn_sum = attn_sum + term.astype(jnp.float32)
    stream = (tokens.astype(jnp.float32) + attn_sum).astype(jnp.bfloat16)
    stream_normed = scaled_rows(stream, mlp_gain)
    gate = jnp.dot(stream_normed, w_gate, preferred_element_type=jnp.float32)
    upward = jnp.dot(stream_normed, w_up, preferred_element_type=jnp.float32)
    hidden = (jax.nn.silu(gate) * upward).astype(jnp.bfloat16)
    block_width = FF // KV_HEADS
    mlp_sum = jnp.zeros((TOKENS, D), jnp.float32)
    for unit_block in range(KV_HEADS):
        lower = unit_block * block_width
        term = jnp.dot(hidden[:, lower:lower + block_width], w_down[lower:lower + block_width], preferred_element_type=jnp.float32)
        term = lax.optimization_barrier(term.astype(jnp.bfloat16))
        mlp_sum = mlp_sum + term.astype(jnp.float32)
    return (stream.astype(jnp.float32) + mlp_sum).astype(jnp.bfloat16)
```

```python
import functools

import jax
import jax.numpy as jnp
from jax import lax
from jax.experimental import pallas as pl
from jax.experimental.pallas import tpu as pltpu
from jax.sharding import Mesh, PartitionSpec as P

HEAD_DIM = 128
WINDOW = 1024
LOG2E = 1.4426950408889634
LANES = 128


def product_t(left, right):
    dims = (((1,), (1,)), ((), ()))
    return lax.dot_general(left, right, dims, preferred_element_type=jnp.float32)


def layer_kernel(
    planes, chips, x_ref, gain1, gain2, attn_w, mlp_w, out_ref,
    afull, mfull, mtrade_ref, held1, held2, nbuf, qbuf, kv, att, hidden,
    given, near, stage, far, stream, leave, arrive,
    at_s, at_r, az_s, az_r, mt_s, mt_r, mz_s, mz_r, loc,
    g_s, g_r, gp_s, gp_r, kv_s, kv_r, zx_s, zx_r, rn_s, rn_r, rf_s, rf_r,
):
    rows, cols = x_ref.shape
    depth = attn_w.shape[1]
    heads_w = qbuf.shape[1]
    qkv_w = heads_w + HEAD_DIM
    gu_w = 2 * hidden.shape[1]
    count = 2 * chips
    h, p, t = lax.axis_index("hi"), lax.axis_index("pair"), lax.axis_index("tensor")
    sib = t + 1 - 2 * lax.rem(t, 2)
    other = 1 - p
    parity = lax.rem(h, 2)
    partner = h + 1 - 2 * parity
    finish = []

    def dev(a, b, c):
        return {"hi": a, "pair": b, "tensor": c}

    def sent(source, target, send, recv, where):
        return pltpu.make_async_remote_copy(
            src_ref=source, dst_ref=target, send_sem=send, recv_sem=recv, device_id=where
        )

    def go(copy, cond=None):
        if cond is None:
            copy.start()
            finish.append(copy.wait_send)
        else:
            pl.when(cond)(lambda: copy.start())
            finish.append(lambda: pl.when(cond)(lambda: copy.wait_send()))

    def ahead(k, start):
        return lax.rem(p + k // chips, 2), lax.rem(start + 2 * (k % chips), count)

    def behind(k, start):
        turn = count - 2 * (k % chips)
        return lax.rem(p + k // chips, 2), lax.rem(start + turn, count)

    barrier = pltpu.get_barrier_semaphore()
    for k in range(1, count):
        there = ahead(k, t)
        pl.semaphore_signal(barrier, inc=1, device_id=dev(h, *there))
    pl.semaphore_signal(barrier, inc=1, device_id=dev(h, p, sib))
    for d in range(1, planes):
        pl.semaphore_signal(barrier, inc=1, device_id=dev(lax.rem(h + d, planes), p, t))
    pl.semaphore_signal(barrier, inc=1, device_id=dev(lax.rem(h + 1, planes), other, t))
    pl.semaphore_signal(barrier, inc=1, device_id=dev(lax.rem(h + planes - 1, planes), other, t))
    pl.semaphore_wait(barrier, count + planes + 1)

    parts = (pl.ds(0, qkv_w), pl.ds(qkv_w, attn_w.shape[2] - qkv_w))
    mparts = (pl.ds(0, gu_w), pl.ds(gu_w, mlp_w.shape[3] - gu_w))

    def at_rows(a, b):
        return pl.ds(pl.multiple_of((a * 2 + b) * depth, depth), depth)

    def atrade(part):
        return sent(
            attn_w.at[other, :, parts[part]],
            afull.at[at_rows(h, p), parts[part]],
            at_s.at[part], at_r.at[part], dev(h, other, t),
        )

    def atrade_wait(part):
        place = afull.at[at_rows(h, other), parts[part]]
        sent(place, place, at_s.at[part], at_r.at[part], dev(h, other, t)).wait_recv()

    def a_slice(src, j, part):
        return afull.at[at_rows(src, j), parts[part]]

    def a_send(k, j, part, own=False):
        for way in range(2):
            src = h - k if way == 0 else h + k
            to = h + 1 if way == 0 else h - 1
            cond = (src >= 0) & (to < planes) if way == 0 else (src < planes) & (to >= 0)
            safe = jnp.clip(src, 0, planes - 1)
            source = attn_w.at[p, :, parts[part]] if own else a_slice(safe, j, part)
            go(
                sent(
                    source, a_slice(safe, j, part),
                    az_s.at[way, k, j, part], az_r.at[safe, j, part],
                    dev(jnp.clip(to, 0, planes - 1), p, t),
                ),
                cond,
            )

    def a_wait(k, part):
        for way in range(2):
            src = h - k if way == 0 else h + k
            cond = src >= 0 if way == 0 else src < planes
            safe = jnp.clip(src, 0, planes - 1)
            for j in range(2):
                place = a_slice(safe, j, part)
                copy = sent(
                    place, place, az_s.at[way, k, j, part], az_r.at[safe, j, part], dev(h, p, t)
                )
                pl.when(cond)(lambda copy=copy: copy.wait_recv())

    def a_relay(k, part):
        a_wait(k, part)
        for j in range(2):
            a_send(k, j, part)

    def block(hold, where):
        return hold.at[
            pl.ds(pl.multiple_of(where[0] * rows, rows), rows),
            pl.ds(pl.multiple_of(where[1] * cols, cols), cols),
        ]

    def gather_start(n, source, hold):
        mine = block(hold, (p, t))
        for k in range(count - 1, 0, -1):
            go(sent(source, mine, g_s.at[n, k], g_r.at[n, k], dev(h, *ahead(k, t))))
        go(sent(source, mine, gp_s.at[n, 0], gp_r.at[n, 0], dev(h, p, sib)))
        pltpu.make_async_copy(source, mine, loc.at[n]).start()

    def gather_pass(n, k, hold):
        came = block(hold, behind(k, t))
        sent(came, came, g_s.at[n, k], g_r.at[n, k], dev(h, p, sib)).wait_recv()
        go(sent(came, came, gp_s.at[n, k], gp_r.at[n, k], dev(h, p, sib)))

    def gather_end(n, source, hold):
        pltpu.make_async_copy(source, block(hold, (p, t)), loc.at[n]).wait()
        for k in range(count):
            came = block(hold, behind(k, sib))
            sent(came, came, gp_s.at[n, k], gp_r.at[n, k], dev(h, p, sib)).wait_recv()

    def mtrade(g, part):
        return sent(
            mlp_w.at[other, g, :, mparts[part]],
            mtrade_ref.at[g, :, mparts[part]],
            mt_s.at[g, part], mt_r.at[g, part], dev(h, other, t),
        )

    def m_slice(src, j, part):
        return mfull.at[at_rows(src, j), mparts[part]]

    def m_send(to, cond, traded, part):
        safe = jnp.clip(to, 0, planes - 1)
        g = lax.rem(safe, 2)
        j = other if traded else p
        source = mtrade_ref.at[g, :, mparts[part]] if traded else mlp_w.at[p, g, :, mparts[part]]
        go(
            sent(
                source, m_slice(h, j, part),
                mz_s.at[safe, j, part], mz_r.at[h, j, part], dev(safe, p, t),
            ),
            cond,
        )

    def m_up(traded, part):
        for d in range(planes - 1, 0, -1):
            m_send(h + d, h + d < planes, traded, part)

    def m_down(traded, part):
        for d in range(planes - 1, 0, -1):
            m_send(h - d, h - d >= 0, traded, part)

    def m_wait(part):
        for d in range(1, planes):
            src = lax.rem(h + d, planes)
            for j in range(2):
                place = m_slice(src, j, part)
                sent(
                    place, place, mz_s.at[src, j, part], mz_r.at[src, j, part], dev(h, p, t)
                ).wait_recv()

    for part in range(2):
        go(atrade(part))
    gather_start(0, x_ref, held1)
    for part in range(2):
        a_send(0, p, part, own=True)
    own_a = pltpu.make_async_copy(attn_w.at[p], afull.at[at_rows(h, p), :], loc.at[3])
    own_m = pltpu.make_async_copy(
        mlp_w.at[p, parity], mfull.at[at_rows(h, p), :], loc.at[4]
    )
    for part in range(2):
        atrade_wait(part)
        a_send(0, other, part)
    own_a.start()
    own_m.start()

    @pl.when(h == 0)
    def _():
        kv[:, 0 : 2 * rows, :] = jnp.zeros((2, 2 * rows, HEAD_DIM), kv.dtype)

    a_relay(1, 0)
    gather_pass(0, 1, held1)
    for k in range(2, planes - 1):
        a_relay(k, 0)
    if planes > 2:
        a_relay(1, 1)
    for k in range(2, count):
        gather_pass(0, k, held1)
    go(mtrade(0, 0))
    m_down(False, 0)
    gather_end(0, x_ref, held1)
    a_wait(planes - 1, 0)
    own_a.wait()

    step = 32
    chunk = nbuf.shape[0]

    def norm_chunk(hold, start, gain):
        @pl.loop(0, chunk // step)
        def _(index):
            source = pl.ds(pl.multiple_of(start + index * step, step), step)
            values = hold[source, :].astype(jnp.float32)
            mean_square = jnp.mean(values * values, axis=1, keepdims=True)
            scaled = values * lax.rsqrt(mean_square + 1e-06) * gain[...]
            nbuf[pl.ds(pl.multiple_of(index * step, step), step), :] = scaled.astype(nbuf.dtype)

    scale = HEAD_DIM ** (-0.5) * LOG2E
    chunks = 2 * rows // chunk

    def kv_copies(i):
        mine = kv.at[p, pl.ds(2 * rows + i * chunk, chunk), :]
        before = kv.at[p, pl.ds(i * chunk, chunk), :]
        up = jnp.minimum(h + 1, planes - 1)
        return (
            sent(mine, before, kv_s.at[1, i], kv_r.at[1, i], dev(up, p, t)),
            sent(mine, before, kv_s.at[2, i], kv_r.at[2, i], dev(up, other, t)),
            sent(mine, mine, kv_s.at[0, i], kv_r.at[0, i], dev(h, other, t)),
        )

    for i in range(chunks):
        norm_chunk(held1, i * chunk, gain1)
        made = jnp.dot(nbuf[...], afull[:, 0:qkv_w], preferred_element_type=jnp.float32)
        qbuf[i * chunk : (i + 1) * chunk, :] = (made[:, :heads_w] * scale).astype(qbuf.dtype)
        kv[p, 2 * rows + i * chunk : 2 * rows + (i + 1) * chunk, :] = made[:, heads_w:].astype(
            kv.dtype
        )
        first, second, across = kv_copies(i)
        go(first, h < planes - 1)
        go(second, h < planes - 1)
        go(across)

    for k in range(2, planes - 1):
        a_relay(k, 1)
    m_up(False, 0)
    go(mtrade(1, 0))
    go(mtrade(0, 1))
    go(mtrade(1, 1))

    def kv_waits(i):
        theirs = kv.at[other, pl.ds(2 * rows + i * chunk, chunk), :]
        sent(theirs, theirs, kv_s.at[0, i], kv_r.at[0, i], dev(h, other, t)).wait_recv()

        @pl.when(h > 0)
        def _():
            for way, which in ((1, p), (2, other)):
                before = kv.at[which, pl.ds(i * chunk, chunk), :]
                sent(before, before, kv_s.at[way, i], kv_r.at[way, i], dev(h, p, t)).wait_recv()

    for i in range(chunks):
        kv_waits(i)

    qrows = 256
    edge = WINDOW

    @pl.loop(0, 2 * rows // qrows)
    def _(i):
        base = pl.multiple_of(i * qrows, qrows)
        for head in range(heads_w // HEAD_DIM):
            lanes = slice(head * HEAD_DIM, (head + 1) * HEAD_DIM)
            q = qbuf[pl.ds(base, qrows), lanes]

            def span(which, lo, size):
                return kv[which, pl.ds(pl.multiple_of(base + lo, qrows), size), :]

            s0 = product_t(q, span(0, 0, qrows))
            s1 = product_t(q, span(0, qrows, edge - qrows))
            s2 = product_t(q, span(0, edge, qrows))
            r = lax.broadcasted_iota(jnp.int32, (qrows, qrows), 0)
            c = lax.broadcasted_iota(jnp.int32, (qrows, qrows), 1)
            s0 = jnp.where((c > r) & (h > 0), s0, -1e30)
            s2 = jnp.where(c <= r, s2, -1e30)
            c1 = lax.broadcasted_iota(jnp.int32, (1, edge - qrows), 1) + (base + qrows)
            s1 = s1 + jnp.where((c1 < edge) & (h == 0), -1e30, 0.0)
            top = jnp.maximum(
                jnp.max(s1, axis=1, keepdims=True),
                jnp.maximum(
                    jnp.max(s0, axis=1, keepdims=True), jnp.max(s2, axis=1, keepdims=True)
                ),
            )
            e0, e1, e2 = (jnp.exp2(s - top) for s in (s0, s1, s2))
            total = (
                jnp.sum(e0, axis=1, keepdims=True)
                + jnp.sum(e1, axis=1, keepdims=True)
                + jnp.sum(e2, axis=1, keepdims=True)
            )
            mixed = jnp.dot(
                e0.astype(jnp.bfloat16), span(1, 0, qrows), preferred_element_type=jnp.float32
            )
            mixed += jnp.dot(
                e1.astype(jnp.bfloat16),
                span(1, qrows, edge - qrows),
                preferred_element_type=jnp.float32,
            )
            mixed += jnp.dot(
                e2.astype(jnp.bfloat16), span(1, edge, qrows), preferred_element_type=jnp.float32
            )
            att[pl.ds(base, qrows), lanes] = (mixed / total).astype(att.dtype)

    half = rows // 2
    nt = 64

    def term(left, first, width, right, lo, where, i):
        part = left[pl.ds(pl.multiple_of(first + where[0] * rows + i * half, half), half), :]
        wide = right[pl.ds(pl.multiple_of(where[1] * cols, cols), cols), lo : lo + width]
        return product_t(part, wide)

    def sums(n, left, first, width, right, lo):
        order = list(range(count - 1, -1, -1))
        for k in order:
            for i in range(2):
                value = term(left, first, width, right, lo, ahead(k, sib), i)
                given[n, k, i * half : (i + 1) * half, :] = value.astype(given.dtype)
            go(sent(given.at[n, k], near.at[n, k], rn_s.at[n, k], rn_r.at[n, k], dev(h, p, sib)))
        for k in order:
            came = near.at[n, k]
            sent(came, came, rn_s.at[n, k], rn_r.at[n, k], dev(h, p, sib)).wait_recv()
            for i in range(2):
                value = term(left, first, width, right, lo, ahead(k, t), i)
                at = slice(i * half, (i + 1) * half)
                value = value + near[n, k, at, :].astype(jnp.float32)
                stage[n, k, at, :] = value.astype(stage.dtype)
            if k:
                go(
                    sent(
                        stage.at[n, k], far.at[n, k], rf_s.at[n, k], rf_r.at[n, k],
                        dev(h, *ahead(k, t)),
                    )
                )

    def sums_end(n, extra, target):
        for k in range(1, count):
            came = far.at[n, k]
            sent(came, came, rf_s.at[n, k], rf_r.at[n, k], dev(h, p, t)).wait_recv()

        @pl.loop(0, rows // nt)
        def _(index):
            part = pl.ds(pl.multiple_of(index * nt, nt), nt)
            total = stage[n, 0, part, :].astype(jnp.float32)
            for k in range(1, count):
                total = total + far[n, k, part, :].astype(jnp.float32)
            for ref in extra:
                total = total + ref[part, :].astype(jnp.float32)
            target[part, :] = total.astype(target.dtype)

    for k in range(1, planes):
        if k == planes - 1 or planes <= 2:
            a_wait(k, 1)
    sums(0, att, 0, heads_w, afull, qkv_w)
    sums_end(0, (x_ref,), stream)

    give = sent(stream, arrive.at[0], zx_s.at[0], zx_r.at[0], dev(partner, p, t))
    go(give)
    gather_start(1, stream, held2.at[0])
    own_m.wait()
    for g in range(2):
        place = mtrade_ref.at[g, :, mparts[0]]
        sent(place, place, mt_s.at[g, 0], mt_r.at[g, 0], dev(h, other, t)).wait_recv()
    m_up(True, 0)
    m_down(True, 0)
    for g in range(2):
        place = mtrade_ref.at[g, :, mparts[1]]
        sent(place, place, mt_s.at[g, 1], mt_r.at[g, 1], dev(h, other, t)).wait_recv()
    kept = pltpu.make_async_copy(
        mtrade_ref.at[parity], mfull.at[at_rows(h, other), :], loc.at[3]
    )
    kept.start()
    for traded in (False, True):
        m_up(traded, 1)
        m_down(traded, 1)
    give.wait_recv()
    gather_start(2, arrive.at[0], held2.at[1])
    for k in range(1, count):
        gather_pass(1, k, held2.at[0])
    gather_end(1, stream, held2.at[0])
    kept.wait()
    m_wait(0)

    units = hidden.shape[1]

    def mlp_chunk(plane, i):
        norm_chunk(held2.at[plane], i * chunk, gain2)
        made = jnp.dot(nbuf[...], mfull[:, 0:gu_w], preferred_element_type=jnp.float32)
        gate, up = made[:, :units], made[:, units:]
        value = gate / (1.0 + jnp.exp(-gate)) * up
        hidden[plane * 2 * rows + i * chunk : plane * 2 * rows + (i + 1) * chunk, :] = value.astype(
            hidden.dtype
        )

    for i in range(chunks):
        mlp_chunk(0, i)
    for k in range(1, count):
        gather_pass(2, k, held2.at[1])
    gather_end(2, arrive.at[0], held2.at[1])
    for i in range(chunks):
        mlp_chunk(1, i)
    m_wait(1)

    sums(1, hidden, 2 * rows, units, mfull, gu_w)
    sums(2, hidden, 0, units, mfull, gu_w)
    sums_end(1, (), leave)
    back = sent(leave, arrive.at[1], zx_s.at[1], zx_r.at[1], dev(partner, p, t))
    go(back)
    for wait in finish[:-1]:
        wait()
    back.wait_recv()
    sums_end(2, (stream, arrive.at[1]), out_ref)
    finish[-1]()


def per_device(tokens, attn_gain, w_query, w_key, w_value, w_out, mlp_gain, w_gate, w_up, w_down):
    rows, cols = tokens.shape
    planes = lax.axis_size("hi")
    chips = lax.axis_size("tensor") // 2
    count = 2 * chips
    depth = w_query.shape[0]
    width = cols * count
    heads_w = w_query.shape[1] // 2
    units = w_gate.shape[1] // 4
    padded = -(-units // LANES) * LANES

    attn_w = []
    for j, extra in enumerate((w_key, w_value)):
        cut = slice(j * heads_w, (j + 1) * heads_w)
        attn_w.append(jnp.concatenate([w_query[:, cut], extra, w_out[cut].T], axis=1))
    attn_w = jnp.stack(attn_w)
    fill = ((0, 0), (0, padded - units))
    mlp_w = []
    for j in range(4):
        cut = slice(j * units, (j + 1) * units)
        pieces = [w_gate[:, cut], w_up[:, cut], w_down[cut].T]
        mlp_w.append(jnp.concatenate([jnp.pad(piece, fill) for piece in pieces], axis=1))
    mlp_w = jnp.stack(mlp_w).reshape(2, 2, depth, 3 * padded)

    bf16 = jnp.bfloat16
    vmem = pl.BlockSpec(memory_space=pltpu.VMEM)
    blocks = pltpu.VMEM((3, count, rows, cols), bf16)
    share = pltpu.VMEM((rows, cols), bf16)
    chunk = rows // 2
    chunks = 2 * rows // chunk
    dma = pltpu.SemaphoreType.DMA
    return pl.pallas_call(
        functools.partial(layer_kernel, planes, chips),
        out_shape=jax.ShapeDtypeStruct((rows, cols), bf16),
        in_specs=[vmem] * 5,
        out_specs=vmem,
        scratch_shapes=[
            pltpu.VMEM((width, attn_w.shape[2]), bf16),
            pltpu.VMEM((width, mlp_w.shape[3]), bf16),
            pltpu.VMEM((2, depth, mlp_w.shape[3]), bf16),
            pltpu.VMEM((2 * rows, width), bf16),
            pltpu.VMEM((2, 2 * rows, width), bf16),
            pltpu.VMEM((chunk, width), bf16),
            pltpu.VMEM((2 * rows, heads_w), bf16),
            pltpu.VMEM((2, 4 * rows, HEAD_DIM), bf16),
            pltpu.VMEM((2 * rows, heads_w), bf16),
            pltpu.VMEM((4 * rows, padded), bf16),
            blocks, blocks, blocks, blocks,
            share, share,
            pltpu.VMEM((2, rows, cols), bf16),
            dma((2,)), dma((2,)),
            dma((2, planes, 2, 2)), dma((planes, 2, 2)),
            dma((2, 2)), dma((2, 2)),
            dma((planes, 2, 2)), dma((planes, 2, 2)),
            dma((5,)),
            dma((3, count)), dma((3, count)), dma((3, count)), dma((3, count)),
            dma((3, chunks)), dma((3, chunks)),
            dma((2,)), dma((2,)),
            dma((3, count)), dma((3, count)), dma((3, count)), dma((3, count)),
        ],
        compiler_params=pltpu.CompilerParams(
            collective_id=1, has_side_effects=True, vmem_limit_bytes=66_000_000
        ),
    )(tokens, attn_gain.reshape(1, -1), mlp_gain.reshape(1, -1), attn_w, mlp_w)


def solution(mesh):
    sizes = mesh.shape
    split = Mesh(
        mesh.devices.reshape(sizes["seq"] // 2, 2, sizes["tensor"]), ("hi", "pair", "tensor")
    )
    seq = ("hi", "pair")
    in_specs = (
        P(seq, "tensor"),
        P(),
        P(seq, "tensor"),
        P(seq, "tensor"),
        P(seq, "tensor"),
        P("tensor", seq),
        P(),
        P(seq, "tensor"),
        P(seq, "tensor"),
        P("tensor", seq),
    )
    return jax.shard_map(
        per_device, mesh=split, in_specs=in_specs, out_specs=P(seq, "tensor"), check_vma=False
    )
```

```python
import functools

import jax
import jax.numpy as jnp
from jax import lax
from jax.experimental import pallas as pl
from jax.experimental.pallas import tpu as pltpu
from jax.sharding import Mesh, PartitionSpec as P

HEAD_DIM = 128
WINDOW = 1024
LOG2E = 1.4426950408889634
LANES = 128


def product_t(left, right):
    dims = (((1,), (1,)), ((), ()))
    return lax.dot_general(left, right, dims, preferred_element_type=jnp.float32)


def layer_kernel(
    planes, chips, x_ref, gain1, gain2, wq, wk, wv, wo, wg, wu, wd, out_ref,
    qkv_full, wo_full, gu_own, gu_full, gu_trade, wd_full, wd_trade, held1, held2, nbuf, qbuf, kv, att, hidden,
    given, near, stage, far, stream, leave, arrive,
    at_s, at_r, az_s, az_r, mt_s, mt_r, mz_s, mz_r, loc, kept,
    g_s, g_r, gp_s, gp_r, kv_s, kv_r, zx_s, zx_r, rn_s, rn_r, rf_s, rf_r,
):
    rows, cols = x_ref.shape
    half = rows // 2
    depth = wq.shape[0]
    heads_w = qbuf.shape[1]
    units, padded = wd.shape[0] // 4, hidden.shape[1]
    gu_w = 2 * padded
    count = 2 * chips
    h, p, t = lax.axis_index("hi"), lax.axis_index("pair"), lax.axis_index("tensor")
    core = lax.rem(t, 2)
    sib = t + 1 - 2 * core
    near_k, far_k = 1 + core, 2 - core
    halves = (pl.ds(0, x_ref.shape[0] // 2), pl.ds(x_ref.shape[0] // 2, x_ref.shape[0] // 2))
    other = 1 - p
    parity = lax.rem(h, 2)
    partner = h + 1 - 2 * parity
    finish = []
    scopes = []

    def mark(name):
        if scopes:
            scopes.pop().__exit__(None, None, None)
        if name:
            scopes.append(jax.named_scope(name))
            scopes[-1].__enter__()

    def dev(a, b, c):
        return {"hi": a, "pair": b, "tensor": c}

    def sent(source, target, send, recv, where):
        return pltpu.make_async_remote_copy(
            src_ref=source, dst_ref=target, send_sem=send, recv_sem=recv, device_id=where
        )

    def go(copy, cond=None):
        if cond is None:
            copy.start()
            finish.append(copy.wait_send)
        else:
            pl.when(cond)(lambda: copy.start())
            finish.append(lambda: pl.when(cond)(lambda: copy.wait_send()))

    def ahead(k, start):
        shift, turn = lax.div(k, 2), lax.rem(k, 2)
        return lax.rem(p + shift, 2), lax.rem(start + 2 * turn, count)

    mark("barrier")
    barrier = pltpu.get_barrier_semaphore()
    for k in range(1, count):
        there = ahead(k, t)
        pl.semaphore_signal(barrier, inc=1, device_id=dev(h, *there))
    pl.semaphore_signal(barrier, inc=1, device_id=dev(h, p, sib))
    for d in range(1, planes):
        pl.semaphore_signal(barrier, inc=1, device_id=dev(lax.rem(h + d, planes), p, t))
    pl.semaphore_signal(barrier, inc=1, device_id=dev(lax.rem(h + 1, planes), other, t))
    pl.semaphore_signal(barrier, inc=1, device_id=dev(lax.rem(h + planes - 1, planes), other, t))
    pl.semaphore_wait(barrier, count + planes + 1)

    def at_rows(a, b):
        return pl.ds(pl.multiple_of((a * 2 + b) * depth, depth), depth)

    def q_cols(which):
        return pl.ds(pl.multiple_of(which * heads_w, heads_w), heads_w)

    def d_rows(which, g):
        return pl.ds(pl.multiple_of((which * 2 + g) * units, 32), units)

    q_place, kv_place = pl.ds(0, heads_w), pl.ds(heads_w, HEAD_DIM)
    across = dev(h, other, t)

    def qkv_trade():
        place = qkv_full.at[at_rows(h, p), :]
        q_copy = sent(wq.at[:, q_cols(other)], place.at[:, q_place], at_s.at[0], at_r.at[0], across)
        k_copy, v_copy = (
            sent(ref, place.at[:, kv_place], at_s.at[1], at_r.at[1], across) for ref in (wk, wv)
        )
        go(q_copy)
        go(k_copy, p == 1)
        go(v_copy, p == 0)

    def qkv_trade_wait():
        place = qkv_full.at[at_rows(h, other), :]
        for n, lanes in ((0, q_place), (1, kv_place)):
            came = place.at[:, lanes]
            sent(came, came, at_s.at[n], at_r.at[n], across).wait_recv()

    def qkv_own():
        place = qkv_full.at[at_rows(h, p), :]
        q_copy = pltpu.make_async_copy(wq.at[:, q_cols(p)], place.at[:, q_place], loc.at[3, 0])
        k_copy, v_copy = (
            pltpu.make_async_copy(ref, place.at[:, kv_place], loc.at[3, 1]) for ref in (wk, wv)
        )
        q_copy.start()
        pl.when(p == 0)(lambda: k_copy.start())
        pl.when(p == 1)(lambda: v_copy.start())
        q_copy.wait()
        k_copy.wait()

    def wo_trade():
        return sent(
            wo.at[q_cols(other), :], wo_full.at[h * 2 + p], at_s.at[2], at_r.at[2], across
        )

    def wo_trade_wait():
        came = wo_full.at[h * 2 + other]
        sent(came, came, at_s.at[2], at_r.at[2], across).wait_recv()

    def a_slice(src, j, part):
        if part:
            return wo_full.at[src * 2 + j]
        return qkv_full.at[at_rows(src, j), :]

    def a_hop(k, way):
        src, to = (h - k, h + 1) if way == 0 else (h + k, h - 1)
        held = src >= 0 if way == 0 else src < planes
        onward = to < planes if way == 0 else to >= 0
        return jnp.clip(src, 0, planes - 1), jnp.clip(to, 0, planes - 1), held, onward

    def a_send(k, j, part, own=False, ways=(0, 1)):
        for way in ways:
            src, to, held, onward = a_hop(k, way)
            source = wo.at[q_cols(p), :] if own and part else a_slice(src, j, part)
            go(
                sent(
                    source, a_slice(src, j, part),
                    az_s.at[way, k, j, part], az_r.at[src, j, part], dev(to, p, t),
                ),
                held & onward,
            )

    def a_wait(k, part, way, last):
        src, to, held, onward = a_hop(k, way)
        cond = held & jnp.logical_not(onward) if last else held & onward
        for j in range(2):
            place = a_slice(src, j, part)
            copy = sent(place, place, az_s.at[way, k, j, part], az_r.at[src, j, part], dev(h, p, t))
            pl.when(cond)(lambda copy=copy: copy.wait_recv())

    def a_relay(k, part):
        for way in range(2):
            a_wait(k, part, way, False)
            for j in range(2):
                a_send(k, j, part, ways=(way,))

    def a_finish(part):
        for k in range(1, planes):
            for way in range(2):
                a_wait(k, part, way, True)

    def block(hold, where, i):
        return hold.at[
            pl.ds(pl.multiple_of(where[0] * rows + i * half, half), half),
            pl.ds(pl.multiple_of(where[1] * cols, cols), cols),
        ]

    def gather_start(n, i, source, hold):
        mine = block(hold, (p, t), i)
        source = source.at[halves[i]]
        for k in (near_k, far_k):
            go(sent(source, mine, g_s.at[n, k, i], g_r.at[n, k, i], dev(h, *ahead(k, t))))
        go(sent(source, mine, gp_s.at[n, 0, i], gp_r.at[n, 0, i], dev(h, p, sib)))
        pltpu.make_async_copy(source, mine, loc.at[n, i]).start()

    def gather_pass(n, i, k, hold, relay=False):
        came = block(hold, ahead(k, t), i)
        sent(came, came, g_s.at[n, k, i], g_r.at[n, k, i], dev(h, p, sib)).wait_recv()
        if relay:
            go(sent(came, came, g_s.at[n, 3, i], g_r.at[n, 3, i], dev(h, *ahead(near_k, t))))
        go(sent(came, came, gp_s.at[n, k, i], gp_r.at[n, k, i], dev(h, p, sib)))

    def gather_relay(n, hold):
        for i in range(2):
            gather_pass(n, i, far_k, hold, relay=True)

    def gather_rest(n, i, source, hold):
        gather_pass(n, i, near_k, hold)
        gather_pass(n, i, 3, hold)
        mine = block(hold, (p, t), i)
        pltpu.make_async_copy(source.at[halves[i]], mine, loc.at[n, i]).wait()
        for k in range(count):
            came = block(hold, ahead(k, sib), i)
            sent(came, came, gp_s.at[n, k, i], gp_r.at[n, k, i], dev(h, p, sib)).wait_recv()

    def mtrade(g, part):
        source = wd.at[d_rows(other, g), :] if part else gu_own.at[other, g]
        target = wd_trade.at[g] if part else gu_trade.at[g]
        return sent(source, target, mt_s.at[g, part], mt_r.at[g, part], across)

    def mtrade_wait(g, part):
        came = wd_trade.at[g] if part else gu_trade.at[g]
        sent(came, came, mt_s.at[g, part], mt_r.at[g, part], across).wait_recv()

    def m_slice(src, j, part):
        if part:
            return wd_full.at[src * 2 + j, pl.ds(0, units), :]
        return gu_full.at[at_rows(src, j), :]

    def m_source(traded, g, part):
        if traded:
            return wd_trade.at[g] if part else gu_trade.at[g]
        return wd.at[d_rows(p, g), :] if part else gu_own.at[p, g]

    def m_send(to, cond, traded, part):
        safe = jnp.clip(to, 0, planes - 1)
        j = other if traded else p
        go(
            sent(
                m_source(traded, lax.rem(safe, 2), part), m_slice(h, j, part),
                mz_s.at[safe, j, part], mz_r.at[h, j, part], dev(safe, p, t),
            ),
            cond,
        )

    def m_keep(traded, part):
        j = other if traded else p
        return pltpu.make_async_copy(
            m_source(traded, parity, part), m_slice(h, j, part), kept.at[int(traded), part]
        )

    def m_up(traded, part, also=True):
        for d in range(planes - 1, 0, -1):
            m_send(h + d, (h + d < planes) & also, traded, part)

    def m_down(traded, part, also=True):
        for d in range(planes - 1, 0, -1):
            m_send(h - d, (h - d >= 0) & also, traded, part)

    def m_outward(traded, part):
        m_up(traded, part, parity == 1)
        m_down(traded, part, parity == 0)

    def m_inward(traded, part):
        m_up(traded, part, parity == 0)
        m_down(traded, part, parity == 1)

    def m_wait(part):
        for traded in (False, True):
            m_keep(traded, part).wait()
        for d in range(1, planes):
            src = lax.rem(h + d, planes)
            for j in range(2):
                place = m_slice(src, j, part)
                sent(
                    place, place, mz_s.at[src, j, part], mz_r.at[src, j, part], dev(h, p, t)
                ).wait_recv()

    def pack():
        zeros = jnp.zeros((depth, padded - units), gu_own.dtype)
        for b in range(4):
            lanes = slice(b * units, (b + 1) * units)
            for n, ref in enumerate((wg, wu)):
                gu_own[b // 2, b % 2, :, n * padded : (n + 1) * padded] = jnp.concatenate(
                    [ref[:, lanes], zeros], axis=1
                )

    mark("start")
    qkv_trade()
    qkv_own()
    a_send(0, p, 0)
    for i in range(2):
        gather_start(0, i, x_ref, held1)
    go(wo_trade())
    mark("pack")
    pack()
    mark("trade")
    qkv_trade_wait()
    a_send(0, other, 0)
    own_wo = pltpu.make_async_copy(wo.at[q_cols(p), :], wo_full.at[h * 2 + p], loc.at[4, 0])
    own_wo.start()
    for part in range(2):
        m_keep(False, part).start()
    for s in range(wd_full.shape[0]):
        wd_full[s, units:, :] = jnp.zeros((padded - units, depth), wd_full.dtype)

    @pl.when(h == 0)
    def _():
        kv[:, 0 : 2 * rows, :] = jnp.zeros((2, 2 * rows, HEAD_DIM), kv.dtype)

    mark("relays")
    a_relay(1, 0)
    gather_relay(0, held1)
    for k in range(2, planes - 1):
        a_relay(k, 0)
    a_send(0, p, 1, own=True)
    wo_trade_wait()
    a_send(0, other, 1)
    mark("gather1")
    go(mtrade(0, 0))
    for i in range(2):
        gather_rest(0, i, x_ref, held1)
    mark("a_wait")
    a_finish(0)

    step = 32
    chunk = nbuf.shape[0]

    def norm_chunk(hold, start, size, gain):
        @pl.loop(0, size // step)
        def _(index):
            source = pl.ds(pl.multiple_of(start + index * step, step), step)
            values = hold[source, :].astype(jnp.float32)
            mean_square = jnp.mean(values * values, axis=1, keepdims=True)
            scaled = values * lax.rsqrt(mean_square + 1e-06) * gain[...]
            nbuf[pl.ds(pl.multiple_of(index * step, step), step), :] = scaled.astype(nbuf.dtype)

    scale = HEAD_DIM ** (-0.5) * LOG2E
    chunks = 2 * rows // chunk

    def kv_rows(first, i):
        return pl.ds(first * 2 * rows + i * chunk, chunk)

    def kv_up(i):
        up = jnp.minimum(h + 1, planes - 1)
        mine, before = kv.at[p, kv_rows(1, i), :], kv.at[p, kv_rows(0, i), :]
        return sent(mine, before, kv_s.at[1, i], kv_r.at[1, i], dev(up, p, t))

    def kv_across(which, first, i):
        mine = kv.at[which, kv_rows(first, i), :]
        slot = 2 * (1 - first)
        return sent(mine, mine, kv_s.at[slot, i], kv_r.at[slot, i], across)

    mark("qkv")
    for i in range(chunks):
        if i == 1:
            a_relay(1, 1)
        norm_chunk(held1, i * chunk, chunk, gain1)
        made = jnp.dot(nbuf[...], qkv_full[...], preferred_element_type=jnp.float32)
        qbuf[i * chunk : (i + 1) * chunk, :] = (made[:, :heads_w] * scale).astype(qbuf.dtype)
        kv[p, 2 * rows + i * chunk : 2 * rows + (i + 1) * chunk, :] = made[:, heads_w:].astype(
            kv.dtype
        )
        go(kv_up(i), h < planes - 1)
        go(kv_across(p, 1, i))

    mark("wo_relay")
    for k in range(2, planes - 1):
        a_relay(k, 1)
    m_down(False, 0)
    m_up(False, 0)

    mark("kv_wait")
    for i in range(chunks):
        pl.when(h > 0)(lambda i=i: kv_up(i).wait_recv())
        go(kv_across(p, 0, i), h > 0)
    for i in range(chunks):
        kv_across(other, 1, i).wait_recv()
        pl.when(h > 0)(lambda i=i: kv_across(other, 0, i).wait_recv())
    go(mtrade(1, 0))
    mark("attention")
    qrows = 256
    edge = WINDOW

    @pl.loop(0, 2 * rows // qrows)
    def _(i):
        base = pl.multiple_of(i * qrows, qrows)
        for head in range(heads_w // HEAD_DIM):
            lanes = slice(head * HEAD_DIM, (head + 1) * HEAD_DIM)
            q = qbuf[pl.ds(base, qrows), lanes]

            def span(which, lo, size):
                return kv[which, pl.ds(pl.multiple_of(base + lo, qrows), size), :]

            s0 = product_t(q, span(0, 0, qrows))
            s1 = product_t(q, span(0, qrows, edge - qrows))
            s2 = product_t(q, span(0, edge, qrows))
            r = lax.broadcasted_iota(jnp.int32, (qrows, qrows), 0)
            c = lax.broadcasted_iota(jnp.int32, (qrows, qrows), 1)
            s0 = jnp.where((c > r) & (h > 0), s0, -1e30)
            s2 = jnp.where(c <= r, s2, -1e30)
            c1 = lax.broadcasted_iota(jnp.int32, (1, edge - qrows), 1) + (base + qrows)
            s1 = s1 + jnp.where((c1 < edge) & (h == 0), -1e30, 0.0)
            top = jnp.maximum(
                jnp.max(s1, axis=1, keepdims=True),
                jnp.maximum(
                    jnp.max(s0, axis=1, keepdims=True), jnp.max(s2, axis=1, keepdims=True)
                ),
            )
            e0, e1, e2 = (jnp.exp2(s - top) for s in (s0, s1, s2))
            total = (
                jnp.sum(e0, axis=1, keepdims=True)
                + jnp.sum(e1, axis=1, keepdims=True)
                + jnp.sum(e2, axis=1, keepdims=True)
            )
            mixed = jnp.dot(
                e0.astype(jnp.bfloat16), span(1, 0, qrows), preferred_element_type=jnp.float32
            )
            mixed += jnp.dot(
                e1.astype(jnp.bfloat16),
                span(1, qrows, edge - qrows),
                preferred_element_type=jnp.float32,
            )
            mixed += jnp.dot(
                e2.astype(jnp.bfloat16), span(1, edge, qrows), preferred_element_type=jnp.float32
            )
            att[pl.ds(base, qrows), lanes] = (mixed / total).astype(att.dtype)

    nt = 64

    def term(left, first, width, right, where, i):
        part = left[pl.ds(pl.multiple_of(first + where[0] * rows + i * half, half), half), :]
        made = [
            jnp.dot(
                part, right[where[1] * (cols // depth) + b], preferred_element_type=jnp.float32
            )
            for b in range(cols // depth)
        ]
        return jnp.concatenate(made, axis=1)

    def give(n, k, left, first, width, right):
        for i in range(2):
            value = term(left, first, width, right, ahead(k, sib), i)
            given[n, k, halves[i], :] = value.astype(given.dtype)
            go(
                sent(
                    given.at[n, k, halves[i]], near.at[n, k, halves[i]],
                    rn_s.at[n, k, i], rn_r.at[n, k, i], dev(h, p, sib),
                )
            )

    def own(n, k, i, extra, left, first, width, right):
        came = near.at[n, k, halves[i]]
        sent(came, came, rn_s.at[n, k, i], rn_r.at[n, k, i], dev(h, p, sib)).wait_recv()
        value = term(left, first, width, right, ahead(k, t), i)
        value = value + near[n, k, halves[i], :].astype(jnp.float32)
        if extra:
            landed(n, 3, i).wait_recv()
            value = value + far[n, 3, halves[i], :].astype(jnp.float32)
        stage[n, k, halves[i], :] = value.astype(stage.dtype)

    def onward(n, k, slot, way, i):
        go(
            sent(
                stage.at[n, k, halves[i]], far.at[n, slot, halves[i]],
                rf_s.at[n, slot, i], rf_r.at[n, slot, i], dev(h, *ahead(way, t)),
            )
        )

    def sums_far(n, *terms):
        give(n, 3, *terms)
        give(n, far_k, *terms)
        for i in range(2):
            own(n, 3, i, False, *terms)
            onward(n, 3, 3, near_k, i)

    def sums_near(n, *terms):
        give(n, near_k, *terms)
        for i in range(2):
            own(n, near_k, i, False, *terms)
            onward(n, near_k, near_k, near_k, i)

    def sums_last(n, *terms):
        give(n, 0, *terms)
        for i in range(2):
            own(n, far_k, i, True, *terms)
            onward(n, far_k, far_k, far_k, i)
        for i in range(2):
            own(n, 0, i, False, *terms)

    def landed(n, k, i):
        came = far.at[n, k, halves[i]]
        return sent(came, came, rf_s.at[n, k, i], rf_r.at[n, k, i], dev(h, p, t))

    def sums_end(n, i, extra, target):
        for k in (1, 2):
            landed(n, k, i).wait_recv()

        @pl.loop(0, half // nt)
        def _(index):
            part = pl.ds(pl.multiple_of(i * half + index * nt, nt), nt)
            total = stage[n, 0, part, :].astype(jnp.float32)
            for k in (1, 2):
                total = total + far[n, k, part, :].astype(jnp.float32)
            for ref in extra:
                total = total + ref[part, :].astype(jnp.float32)
            target[part, :] = total.astype(target.dtype)

    mark("trade_wait")
    for g in range(2):
        mtrade_wait(g, 0)
    m_keep(True, 0).start()
    m_outward(True, 0)
    m_outward(False, 1)
    mark("wo_wait")
    a_finish(1)
    mark("sums0")
    own_wo.wait()
    sums_far(0, att, 0, heads_w, wo_full)
    sums_near(0, att, 0, heads_w, wo_full)
    sums_last(0, att, 0, heads_w, wo_full)
    go(mtrade(0, 1))
    go(mtrade(1, 1))
    mark("end0")
    gives = []
    for i in range(2):
        sums_end(0, i, (x_ref,), stream)
        gives.append(
            sent(
                stream.at[halves[i]], arrive.at[0, halves[i]],
                zx_s.at[0, i], zx_r.at[0, i], dev(partner, p, t),
            )
        )
        go(gives[i])
        gather_start(1, i, stream, held2.at[0])
    mark("send2")
    m_inward(True, 0)
    m_inward(False, 1)
    for g in range(2):
        mtrade_wait(g, 1)
    m_keep(True, 1).start()
    m_outward(True, 1)
    m_inward(True, 1)
    mark("zwait")
    gather_relay(1, held2.at[0])
    mark("gather2a")
    for i in range(2):
        gives[i].wait_recv()
        gather_start(2, i, arrive.at[0], held2.at[1])
    for i in range(2):
        gather_rest(1, i, stream, held2.at[0])
    mark("relay2b")
    gather_relay(2, held2.at[1])
    mark("gu_wait")
    m_wait(0)


    def mlp_half(plane, i):
        for run in range(2):
            start = run * rows + i * half
            norm_chunk(held2.at[plane], start, half, gain2)
            made = jnp.dot(nbuf[0:half, :], gu_full[...], preferred_element_type=jnp.float32)
            gate, up = made[:, :padded], made[:, padded:]
            value = gate / (1.0 + jnp.exp(-gate)) * up
            start = plane * 2 * rows + start
            hidden[start : start + half, :] = value.astype(hidden.dtype)

    mark("mlp0")
    for i in range(2):
        mlp_half(0, i)
    for i in range(2):
        mark("gather2b")
        gather_rest(2, i, arrive.at[0], held2.at[1])
        mark("mlp1")
        mlp_half(1, i)
    mark("wd_wait")
    m_wait(1)

    mark("sums1")
    theirs = (1, hidden, 2 * rows, padded, wd_full)
    ours = (2, hidden, 0, padded, wd_full)
    sums_far(*theirs)
    sums_near(*theirs)
    sums_far(*ours)
    mark("sums2")
    sums_last(*theirs)
    sums_near(*ours)
    mark("sums3")
    sums_last(*ours)
    mark("end1")
    backs = []
    for i in range(2):
        sums_end(1, i, (), leave)
        backs.append(
            sent(
                leave.at[halves[i]], arrive.at[1, halves[i]],
                zx_s.at[1, i], zx_r.at[1, i], dev(partner, p, t),
            )
        )
        go(backs[i])
    mark("end2")
    for i in range(2):
        backs[i].wait_recv()
        sums_end(2, i, (stream, arrive.at[1]), out_ref)
    mark("drain")
    for wait in finish:
        wait()
    mark(None)


def per_device(tokens, attn_gain, w_query, w_key, w_value, w_out, mlp_gain, w_gate, w_up, w_down):
    rows, cols = tokens.shape
    planes = lax.axis_size("hi")
    chips = lax.axis_size("tensor") // 2
    count = 2 * chips
    depth = w_query.shape[0]
    width = cols * count
    heads_w = w_query.shape[1] // 2
    units = w_gate.shape[1] // 4
    padded = -(-units // LANES) * LANES

    bf16 = jnp.bfloat16
    vmem = pl.BlockSpec(memory_space=pltpu.VMEM)
    blocks = pltpu.VMEM((3, count, rows, cols), bf16)
    share = pltpu.VMEM((rows, cols), bf16)
    chunk = rows // 2
    chunks = 2 * rows // chunk
    dma = pltpu.SemaphoreType.DMA
    return pl.pallas_call(
        functools.partial(layer_kernel, planes, chips),
        out_shape=jax.ShapeDtypeStruct((rows, cols), bf16),
        in_specs=[vmem] * 10,
        out_specs=vmem,
        scratch_shapes=[
            pltpu.VMEM((width, heads_w + HEAD_DIM), bf16),
            pltpu.VMEM((2 * planes, heads_w, depth), bf16),
            pltpu.VMEM((2, 2, depth, 2 * padded), bf16),
            pltpu.VMEM((width, 2 * padded), bf16),
            pltpu.VMEM((2, depth, 2 * padded), bf16),
            pltpu.VMEM((2 * planes, padded, depth), bf16),
            pltpu.VMEM((2, units, depth), bf16),
            pltpu.VMEM((2 * rows, width), bf16),
            pltpu.VMEM((2, 2 * rows, width), bf16),
            pltpu.VMEM((chunk, width), bf16),
            pltpu.VMEM((2 * rows, heads_w), bf16),
            pltpu.VMEM((2, 4 * rows, HEAD_DIM), bf16),
            pltpu.VMEM((2 * rows, heads_w), bf16),
            pltpu.VMEM((4 * rows, padded), bf16),
            blocks, blocks, blocks, blocks,
            share, share,
            pltpu.VMEM((2, rows, cols), bf16),
            dma((3,)), dma((3,)),
            dma((2, planes, 2, 2)), dma((planes, 2, 2)),
            dma((2, 2)), dma((2, 2)),
            dma((planes, 2, 2)), dma((planes, 2, 2)),
            dma((5, 2)), dma((2, 2)),
            dma((3, count, 2)), dma((3, count, 2)), dma((3, count, 2)), dma((3, count, 2)),
            dma((3, chunks)), dma((3, chunks)),
            dma((2, 2)), dma((2, 2)),
            dma((3, count, 2)), dma((3, count, 2)), dma((3, count, 2)), dma((3, count, 2)),
        ],
        compiler_params=pltpu.CompilerParams(
            collective_id=1, has_side_effects=True, vmem_limit_bytes=66_000_000
        ),
    )(
        tokens, attn_gain.reshape(1, -1), mlp_gain.reshape(1, -1),
        w_query, w_key, w_value, w_out, w_gate, w_up, w_down,
    )


def solution(mesh):
    sizes = mesh.shape
    split = Mesh(
        mesh.devices.reshape(sizes["seq"] // 2, 2, sizes["tensor"]), ("hi", "pair", "tensor")
    )
    seq = ("hi", "pair")
    in_specs = (
        P(seq, "tensor"),
        P(),
        P(seq, "tensor"),
        P(seq, "tensor"),
        P(seq, "tensor"),
        P("tensor", seq),
        P(),
        P(seq, "tensor"),
        P(seq, "tensor"),
        P("tensor", seq),
    )
    return jax.shard_map(
        per_device, mesh=split, in_specs=in_specs, out_specs=P(seq, "tensor"), check_vma=False
    )
```

```python
import functools

import jax
import jax.numpy as jnp
from jax import lax
from jax.experimental import pallas as pl
from jax.experimental.pallas import tpu as pltpu
from jax.sharding import Mesh, PartitionSpec as P

HEAD_DIM = 128
WINDOW = 1024
LOG2E = 1.4426950408889634
LANES = 128


def product_t(left, right):
    dims = (((1,), (1,)), ((), ()))
    return lax.dot_general(left, right, dims, preferred_element_type=jnp.float32)


def layer_kernel(
    planes, chips, x_ref, gain1, gain2, wq, wk, wv, wo, wg, wu, wd, out_ref,
    qkv_full, wo_full, gu_own, gu_full, gu_trade, wd_full, wd_trade, held1, held2, nbuf, qbuf, kv, hidden,
    given, near, stage, far, stream, leave, arrive,
    at_s, at_r, az_s, az_r, mt_s, mt_r, mz_s, mz_r, loc, kept,
    g_s, g_r, gp_s, gp_r, kv_s, kv_r, zx_s, zx_r, rn_s, rn_r, rf_s, rf_r,
):
    rows, cols = x_ref.shape
    half = rows // 2
    depth = wq.shape[0]
    heads_w = qbuf.shape[1]
    units, padded = wd.shape[0] // 4, hidden.shape[1]
    aligned = depth % LANES == 0
    count = 2 * chips
    h, p, t = lax.axis_index("hi"), lax.axis_index("pair"), lax.axis_index("tensor")
    core = lax.rem(t, 2)
    sib = t + 1 - 2 * core
    near_k, far_k = 1 + core, 2 - core
    halves = (pl.ds(0, x_ref.shape[0] // 2), pl.ds(x_ref.shape[0] // 2, x_ref.shape[0] // 2))
    other = 1 - p
    parity = lax.rem(h, 2)
    partner = h + 1 - 2 * parity
    finish = []
    scopes = []

    def mark(name):
        if scopes:
            scopes.pop().__exit__(None, None, None)
        if name:
            scopes.append(jax.named_scope(name))
            scopes[-1].__enter__()

    def dev(a, b, c):
        return {"hi": a, "pair": b, "tensor": c}

    def sent(source, target, send, recv, where):
        return pltpu.make_async_remote_copy(
            src_ref=source, dst_ref=target, send_sem=send, recv_sem=recv, device_id=where
        )

    def go(copy, cond=None):
        if cond is None:
            copy.start()
            finish.append(copy.wait_send)
        else:
            pl.when(cond)(lambda: copy.start())
            finish.append(lambda: pl.when(cond)(lambda: copy.wait_send()))

    def ahead(k, start):
        shift, turn = lax.div(k, 2), lax.rem(k, 2)
        return lax.rem(p + shift, 2), lax.rem(start + 2 * turn, count)

    mark("barrier")
    barrier = pltpu.get_barrier_semaphore()
    for k in range(1, count):
        there = ahead(k, t)
        pl.semaphore_signal(barrier, inc=1, device_id=dev(h, *there))
    pl.semaphore_signal(barrier, inc=1, device_id=dev(h, p, sib))
    for d in range(1, planes):
        pl.semaphore_signal(barrier, inc=1, device_id=dev(lax.rem(h + d, planes), p, t))
    pl.semaphore_signal(barrier, inc=1, device_id=dev(lax.rem(h + 1, planes), other, t))
    pl.semaphore_signal(barrier, inc=1, device_id=dev(lax.rem(h + planes - 1, planes), other, t))
    pl.semaphore_wait(barrier, count + planes + 1)

    def at_rows(a, b):
        return pl.ds(pl.multiple_of((a * 2 + b) * depth, depth), depth)

    def q_cols(which):
        return pl.ds(pl.multiple_of(which * heads_w, heads_w), heads_w)

    def d_rows(which, g):
        return pl.ds(pl.multiple_of((which * 2 + g) * units, 32), units)

    q_place, kv_place = pl.ds(0, heads_w), pl.ds(heads_w, HEAD_DIM)
    across = dev(h, other, t)

    def qkv_trade():
        place = qkv_full.at[at_rows(h, p), :]
        q_copy = sent(wq.at[:, q_cols(other)], place.at[:, q_place], at_s.at[0], at_r.at[0], across)
        k_copy, v_copy = (
            sent(ref, place.at[:, kv_place], at_s.at[1], at_r.at[1], across) for ref in (wk, wv)
        )
        go(q_copy)
        go(k_copy, p == 1)
        go(v_copy, p == 0)

    def qkv_trade_wait():
        place = qkv_full.at[at_rows(h, other), :]
        for n, lanes in ((0, q_place), (1, kv_place)):
            came = place.at[:, lanes]
            sent(came, came, at_s.at[n], at_r.at[n], across).wait_recv()

    def qkv_own():
        place = qkv_full.at[at_rows(h, p), :]
        q_copy = pltpu.make_async_copy(wq.at[:, q_cols(p)], place.at[:, q_place], loc.at[3, 0])
        k_copy, v_copy = (
            pltpu.make_async_copy(ref, place.at[:, kv_place], loc.at[3, 1]) for ref in (wk, wv)
        )
        q_copy.start()
        pl.when(p == 0)(lambda: k_copy.start())
        pl.when(p == 1)(lambda: v_copy.start())
        q_copy.wait()
        k_copy.wait()

    def wo_trade():
        return sent(
            wo.at[q_cols(other), :], wo_full.at[h * 2 + p], at_s.at[2], at_r.at[2], across
        )

    def wo_trade_wait():
        came = wo_full.at[h * 2 + other]
        sent(came, came, at_s.at[2], at_r.at[2], across).wait_recv()

    def a_slice(src, j, part):
        if part:
            return wo_full.at[src * 2 + j]
        return qkv_full.at[at_rows(src, j), :]

    def a_hop(k, way):
        src, to = (h - k, h + 1) if way == 0 else (h + k, h - 1)
        held = src >= 0 if way == 0 else src < planes
        onward = to < planes if way == 0 else to >= 0
        return jnp.clip(src, 0, planes - 1), jnp.clip(to, 0, planes - 1), held, onward

    def a_send(k, j, part, own=False, ways=(0, 1)):
        for way in ways:
            src, to, held, onward = a_hop(k, way)
            source = wo.at[q_cols(p), :] if own and part else a_slice(src, j, part)
            go(
                sent(
                    source, a_slice(src, j, part),
                    az_s.at[way, k, j, part], az_r.at[src, j, part], dev(to, p, t),
                ),
                held & onward,
            )

    def a_wait(k, part, way, last):
        src, to, held, onward = a_hop(k, way)
        cond = held & jnp.logical_not(onward) if last else held & onward
        for j in range(2):
            place = a_slice(src, j, part)
            copy = sent(place, place, az_s.at[way, k, j, part], az_r.at[src, j, part], dev(h, p, t))
            pl.when(cond)(lambda copy=copy: copy.wait_recv())

    def a_relay(k, part, ways=(0, 1)):
        for way in ways:
            a_wait(k, part, way, False)
            for j in range(2):
                a_send(k, j, part, ways=(way,))

    def a_finish(part):
        for k in range(1, planes):
            for way in range(2):
                a_wait(k, part, way, True)

    def block(hold, where, i):
        return hold.at[
            pl.ds(pl.multiple_of(where[0] * rows + i * half, half), half),
            pl.ds(pl.multiple_of(where[1] * cols, cols), cols),
        ]

    def gather_start(n, i, source, hold):
        mine = block(hold, (p, t), i)
        source = source.at[halves[i]]
        for k in (near_k, far_k):
            go(sent(source, mine, g_s.at[n, k, i], g_r.at[n, k, i], dev(h, *ahead(k, t))))
        go(sent(source, mine, gp_s.at[n, 0, i], gp_r.at[n, 0, i], dev(h, p, sib)))
        pltpu.make_async_copy(source, mine, loc.at[n, i]).start()

    def gather_pass(n, i, k, hold, relay=False):
        came = block(hold, ahead(k, t), i)
        sent(came, came, g_s.at[n, k, i], g_r.at[n, k, i], dev(h, p, sib)).wait_recv()
        if relay:
            go(sent(came, came, g_s.at[n, 3, i], g_r.at[n, 3, i], dev(h, *ahead(near_k, t))))
        go(sent(came, came, gp_s.at[n, k, i], gp_r.at[n, k, i], dev(h, p, sib)))

    def gather_relay(n, hold):
        for i in range(2):
            gather_pass(n, i, far_k, hold, relay=True)

    def gather_rest(n, i, source, hold):
        gather_pass(n, i, near_k, hold)
        gather_pass(n, i, 3, hold)
        mine = block(hold, (p, t), i)
        pltpu.make_async_copy(source.at[halves[i]], mine, loc.at[n, i]).wait()
        for k in range(count):
            came = block(hold, ahead(k, sib), i)
            sent(came, came, gp_s.at[n, k, i], gp_r.at[n, k, i], dev(h, p, sib)).wait_recv()

    def mtrade(g, part):
        source = wd.at[d_rows(other, g), :] if part else gu_own.at[other, g]
        target = wd_trade.at[g] if part else gu_trade.at[g]
        return sent(source, target, mt_s.at[g, part], mt_r.at[g, part], across)

    def mtrade_wait(g, part):
        came = wd_trade.at[g] if part else gu_trade.at[g]
        sent(came, came, mt_s.at[g, part], mt_r.at[g, part], across).wait_recv()

    def m_slice(src, j, part):
        if part:
            return wd_full.at[src * 2 + j, pl.ds(0, units), :]
        if aligned:
            lanes = pl.ds(pl.multiple_of((src * 2 + j) * depth, depth), depth)
            return gu_full.at[:, pl.ds(0, units), lanes]
        return gu_full.at[at_rows(src, j), :]

    def m_source(traded, g, part):
        if traded:
            return wd_trade.at[g] if part else gu_trade.at[g]
        return wd.at[d_rows(p, g), :] if part else gu_own.at[p, g]

    def m_send(to, cond, traded, part):
        safe = jnp.clip(to, 0, planes - 1)
        j = other if traded else p
        go(
            sent(
                m_source(traded, lax.rem(safe, 2), part), m_slice(h, j, part),
                mz_s.at[safe, j, part], mz_r.at[h, j, part], dev(safe, p, t),
            ),
            cond,
        )

    def m_keep(traded, part):
        j = other if traded else p
        return pltpu.make_async_copy(
            m_source(traded, parity, part), m_slice(h, j, part), kept.at[int(traded), part]
        )

    def m_up(traded, part, also=True, steps=None):
        for d in steps or range(planes - 1, 0, -1):
            m_send(h + d, (h + d < planes) & also, traded, part)

    def m_down(traded, part, also=True, steps=None):
        for d in steps or range(planes - 1, 0, -1):
            m_send(h - d, (h - d >= 0) & also, traded, part)

    def m_outward(traded, part, steps=None):
        m_up(traded, part, parity == 1, steps)
        m_down(traded, part, parity == 0, steps)

    def m_inward(traded, part):
        m_up(traded, part, parity == 0)
        m_down(traded, part, parity == 1)

    def m_wait(part):
        for traded in (False, True):
            m_keep(traded, part).wait()
        for d in range(1, planes):
            src = lax.rem(h + d, planes)
            for j in range(2):
                place = m_slice(src, j, part)
                sent(
                    place, place, mz_s.at[src, j, part], mz_r.at[src, j, part], dev(h, p, t)
                ).wait_recv()

    def pack():
        for n, ref in enumerate((wg, wu)):
            turned = ref[...].T if aligned else ref[...]
            for b in range(4):
                cut = slice(b * units, (b + 1) * units)
                if aligned:
                    gu_own[b // 2, b % 2, n] = turned[cut]
                else:
                    gu_own[b // 2, b % 2, :, n * padded : (n + 1) * padded] = jnp.pad(
                        turned[:, cut], ((0, 0), (0, padded - units))
                    )
        if aligned:
            gu_full[:, units:, :] = jnp.zeros((2, padded - units, gu_full.shape[2]), gu_full.dtype)

    def gate_up(left):
        if aligned:
            return product_t(left, gu_full[...].reshape(2 * padded, gu_full.shape[2]))
        return jnp.dot(left, gu_full[...], preferred_element_type=jnp.float32)

    step = 32

    def norm_half(hold, gain, i, put):
        @pl.loop(0, 2 * half // step)
        def _(index):
            run, at = lax.div(index, half // step), lax.rem(index, half // step)
            source = pl.ds(pl.multiple_of(run * rows + i * half + at * step, step), step)
            target = source
            if put is None:
                target = pl.ds(pl.multiple_of(index * step, step), step)
            values = hold[source, :].astype(jnp.float32)
            mean_square = jnp.mean(values * values, axis=1, keepdims=True)
            scaled = values * lax.rsqrt(mean_square + 1e-06) * gain[...]
            nbuf[target, :] = scaled.astype(nbuf.dtype)

    mark("start")
    qkv_trade()
    qkv_own()
    a_send(0, p, 0)
    for i in range(2):
        gather_start(0, i, x_ref, held1)
    go(wo_trade())
    mark("pack")
    pack()
    mark("trade")
    qkv_trade_wait()
    a_send(0, other, 0)
    own_wo = pltpu.make_async_copy(wo.at[q_cols(p), :], wo_full.at[h * 2 + p], loc.at[4, 0])
    own_wo.start()
    for part in range(2):
        m_keep(False, part).start()
    for s in range(wd_full.shape[0]):
        wd_full[s, units:, :] = jnp.zeros((padded - units, depth), wd_full.dtype)

    @pl.when(h == 0)
    def _():
        kv[:, 0 : 2 * rows, :] = jnp.zeros((2, 2 * rows, HEAD_DIM), kv.dtype)

    mark("relays")
    a_relay(1, 0)
    gather_relay(0, held1)
    for k in range(2, planes - 1):
        a_relay(k, 0)
    a_send(0, p, 1, own=True)
    wo_trade_wait()
    a_send(0, other, 1)
    mark("gather1")
    go(mtrade(0, 0))
    for i in range(2):
        gather_rest(0, i, x_ref, held1)
        norm_half(held1, gain1, i, 0)
    mark("a_wait")
    a_finish(0)

    chunk = rows // 2
    scale = HEAD_DIM ** (-0.5) * LOG2E
    chunks = 2 * rows // chunk

    def kv_rows(first, i):
        return pl.ds(first * 2 * rows + i * chunk, chunk)

    def kv_up(i):
        up = jnp.minimum(h + 1, planes - 1)
        mine, before = kv.at[p, kv_rows(1, i), :], kv.at[p, kv_rows(0, i), :]
        return sent(mine, before, kv_s.at[1, i], kv_r.at[1, i], dev(up, p, t))

    def kv_across(which, first, i):
        mine = kv.at[which, kv_rows(first, i), :]
        slot = 2 * (1 - first)
        return sent(mine, mine, kv_s.at[slot, i], kv_r.at[slot, i], across)

    mark("qkv")
    for i in range(chunks):
        if i == 1:
            a_relay(1, 1, ways=(1,))
        made = jnp.dot(nbuf[i * chunk : (i + 1) * chunk, :], qkv_full[...], preferred_element_type=jnp.float32)
        qbuf[i * chunk : (i + 1) * chunk, :] = (made[:, :heads_w] * scale).astype(qbuf.dtype)
        kv[p, 2 * rows + i * chunk : 2 * rows + (i + 1) * chunk, :] = made[:, heads_w:].astype(
            kv.dtype
        )
        go(kv_up(i), h < planes - 1)
        go(kv_across(p, 1, i))

    mark("wo_relay")
    a_relay(1, 1, ways=(0,))
    for k in range(2, planes - 1):
        a_relay(k, 1)

    mark("kv_wait")
    for i in range(chunks):
        pl.when(h > 0)(lambda i=i: kv_up(i).wait_recv())
        go(kv_across(p, 0, i), h > 0)
    for i in range(chunks):
        kv_across(other, 1, i).wait_recv()
        pl.when(h > 0)(lambda i=i: kv_across(other, 0, i).wait_recv())
    go(mtrade(1, 0))
    m_down(False, 0)
    mark("attention")
    qrows = 256
    edge = WINDOW

    @pl.loop(0, 2 * rows // qrows)
    def _(i):
        base = pl.multiple_of(i * qrows, qrows)
        for head in range(heads_w // HEAD_DIM):
            lanes = slice(head * HEAD_DIM, (head + 1) * HEAD_DIM)
            q = qbuf[pl.ds(base, qrows), lanes]

            def span(which, lo, size):
                return kv[which, pl.ds(pl.multiple_of(base + lo, qrows), size), :]

            s0 = product_t(q, span(0, 0, qrows))
            s1 = product_t(q, span(0, qrows, edge - qrows))
            s2 = product_t(q, span(0, edge, qrows))
            r = lax.broadcasted_iota(jnp.int32, (qrows, qrows), 0)
            c = lax.broadcasted_iota(jnp.int32, (qrows, qrows), 1)
            s0 = jnp.where((c > r) & (h > 0), s0, -1e30)
            s2 = jnp.where(c <= r, s2, -1e30)
            c1 = lax.broadcasted_iota(jnp.int32, (1, edge - qrows), 1) + (base + qrows)
            s1 = s1 + jnp.where((c1 < edge) & (h == 0), -1e30, 0.0)
            top = jnp.maximum(
                jnp.max(s1, axis=1, keepdims=True),
                jnp.maximum(
                    jnp.max(s0, axis=1, keepdims=True), jnp.max(s2, axis=1, keepdims=True)
                ),
            )
            e0, e1, e2 = (jnp.exp2(s - top) for s in (s0, s1, s2))
            total = (
                jnp.sum(e0, axis=1, keepdims=True)
                + jnp.sum(e1, axis=1, keepdims=True)
                + jnp.sum(e2, axis=1, keepdims=True)
            )
            mixed = jnp.dot(
                e0.astype(jnp.bfloat16), span(1, 0, qrows), preferred_element_type=jnp.float32
            )
            mixed += jnp.dot(
                e1.astype(jnp.bfloat16),
                span(1, qrows, edge - qrows),
                preferred_element_type=jnp.float32,
            )
            mixed += jnp.dot(
                e2.astype(jnp.bfloat16), span(1, edge, qrows), preferred_element_type=jnp.float32
            )
            qbuf[pl.ds(base, qrows), lanes] = (mixed / total).astype(qbuf.dtype)

    nt = 64

    def term(left, first, width, right, where, i):
        part = left[pl.ds(pl.multiple_of(first + where[0] * rows + i * half, half), half), :]
        made = [
            jnp.dot(
                part, right[where[1] * (cols // depth) + b], preferred_element_type=jnp.float32
            )
            for b in range(cols // depth)
        ]
        return jnp.concatenate(made, axis=1)

    given_sends = {}

    def give(n, k, left, first, width, right):
        slot = n % 2
        for i in range(2):
            before = given_sends.pop((slot, id(k), i), None)
            if before is not None:
                before()
                finish[:] = [wait for wait in finish if wait is not before]
            value = term(left, first, width, right, ahead(k, sib), i)
            given[slot, k, halves[i], :] = value.astype(given.dtype)
            go(
                sent(
                    given.at[slot, k, halves[i]], near.at[n, k, halves[i]],
                    rn_s.at[n, k, i], rn_r.at[n, k, i], dev(h, p, sib),
                )
            )
            given_sends[slot, id(k), i] = finish[-1]

    def own(n, k, i, extra, left, first, width, right):
        came = near.at[n, k, halves[i]]
        sent(came, came, rn_s.at[n, k, i], rn_r.at[n, k, i], dev(h, p, sib)).wait_recv()
        value = term(left, first, width, right, ahead(k, t), i)
        value = value + near[n, k, halves[i], :].astype(jnp.float32)
        if extra is not None:
            landed(*extra, i).wait_recv()
            value = value + far[extra[0], extra[1] - 1, halves[i], :].astype(jnp.float32)
        stage[n, k, halves[i], :] = value.astype(stage.dtype)

    def onward(n, k, slot, way, i):
        go(
            sent(
                stage.at[n, k, halves[i]], far.at[n, slot - 1, halves[i]],
                rf_s.at[n, slot, i], rf_r.at[n, slot, i], dev(h, *ahead(way, t)),
            )
        )

    def sums_far(n, over, *terms):
        if over != "join":
            give(n, 3, *terms)
            give(n, far_k, *terms)
        for i in range(2):
            own(n, 3, i, (1, 3) if over == "join" else None, *terms)
            if over == "leave":
                go(
                    sent(
                        stage.at[n, 3, halves[i]], far.at[n, 2, halves[i]],
                        rf_s.at[n, 3, i], rf_r.at[n, 3, i], dev(partner, p, t),
                    )
                )
            else:
                onward(n, 3, 3, near_k, i)

    def sums_near(n, *terms):
        give(n, near_k, *terms)
        for i in range(2):
            own(n, near_k, i, None, *terms)
            onward(n, near_k, near_k, near_k, i)

    def sums_last(n, relayed, *terms):
        give(n, 0, *terms)
        for i in range(2):
            own(n, far_k, i, (n, 3) if relayed else None, *terms)
            onward(n, far_k, far_k, far_k, i)
        for i in range(2):
            own(n, 0, i, None, *terms)

    def landed(n, k, i):
        came = far.at[n, k - 1, halves[i]]
        return sent(came, came, rf_s.at[n, k, i], rf_r.at[n, k, i], dev(h, p, t))

    def sums_end(n, i, extra, target):
        for k in (1, 2):
            landed(n, k, i).wait_recv()

        @pl.loop(0, half // nt)
        def _(index):
            part = pl.ds(pl.multiple_of(i * half + index * nt, nt), nt)
            total = stage[n, 0, part, :].astype(jnp.float32)
            for k in (1, 2):
                total = total + far[n, k - 1, part, :].astype(jnp.float32)
            for ref in extra:
                total = total + ref[part, :].astype(jnp.float32)
            target[part, :] = total.astype(target.dtype)

    m_up(False, 0)
    mark("trade_wait")
    for g in range(2):
        mtrade_wait(g, 0)
    m_keep(True, 0).start()
    m_outward(True, 0)
    mark("wo_wait")
    a_finish(1)
    mark("sums0")
    own_wo.wait()
    sums_far(0, None, qbuf, 0, heads_w, wo_full)
    sums_near(0, qbuf, 0, heads_w, wo_full)
    sums_last(0, True, qbuf, 0, heads_w, wo_full)
    mark("end0")
    gives = []
    for i in range(2):
        sums_end(0, i, (x_ref,), stream)
        gives.append(
            sent(
                stream.at[halves[i]], arrive.at[0, halves[i]],
                zx_s.at[0, i], zx_r.at[0, i], dev(partner, p, t),
            )
        )
        go(gives[i])
        gather_start(1, i, stream, held2.at[0])
    mark("send2")
    m_inward(True, 0)
    m_outward(False, 1)
    m_inward(False, 1)
    mark("zwait")
    gather_relay(1, held2.at[0])
    go(mtrade(0, 1))
    go(mtrade(1, 1))
    mark("gather2a")
    for i in range(2):
        gives[i].wait_recv()
        gather_start(2, i, arrive.at[0], held2.at[1])
    for i in range(2):
        gather_rest(1, i, stream, held2.at[0])
        norm_half(held2.at[0], gain2, i, 0)
    mark("wd_trade")
    for g in range(2):
        mtrade_wait(g, 1)
    m_keep(True, 1).start()
    m_outward(True, 1)
    m_inward(True, 1)
    mark("relay2b")
    gather_relay(2, held2.at[1])
    mark("gu_wait")
    m_wait(0)


    def mlp_rows(start, put):
        made = gate_up(nbuf[put : put + rows, :])
        gate, up = made[:, :padded], made[:, padded:]
        value = (gate / (1.0 + jnp.exp(-gate)) * up).astype(hidden.dtype)
        for at, size, first in start:
            hidden[at : at + size, :] = value[first : first + size]

    mark("mlp0")
    for run in range(2):
        mlp_rows(((run * rows, rows, 0),), run * rows)
    for i in range(2):
        mark("gather2b")
        gather_rest(2, i, arrive.at[0], held2.at[1])
        mark("mlp1")
        norm_half(held2.at[1], gain2, i, None)
        first = 2 * rows + i * half
        mlp_rows(((first, half, 0), (first + rows, half, half)), 0)
    mark("wd_wait")
    m_wait(1)

    mark("sums1")
    theirs = (hidden, 2 * rows, padded, wd_full)
    ours = (hidden, 0, padded, wd_full)
    sums_far(1, "leave", *theirs)
    sums_near(1, *theirs)
    mark("sums2")
    sums_last(1, False, *theirs)
    for k in (3, far_k):
        give(2, k, *ours)
    mark("sums3")
    sums_far(2, "join", *ours)
    sums_near(2, *ours)
    mark("end1")
    backs = []
    for i in range(2):
        sums_end(1, i, (), leave)
        backs.append(
            sent(
                leave.at[halves[i]], arrive.at[1, halves[i]],
                zx_s.at[1, i], zx_r.at[1, i], dev(partner, p, t),
            )
        )
        go(backs[i])
    mark("sums4")
    sums_last(2, True, *ours)
    mark("end2")
    for i in range(2):
        backs[i].wait_recv()
        sums_end(2, i, (stream, arrive.at[1]), out_ref)
    mark("drain")
    for wait in finish:
        wait()
    mark(None)


def per_device(tokens, attn_gain, w_query, w_key, w_value, w_out, mlp_gain, w_gate, w_up, w_down):
    rows, cols = tokens.shape
    planes = lax.axis_size("hi")
    chips = lax.axis_size("tensor") // 2
    count = 2 * chips
    depth = w_query.shape[0]
    width = cols * count
    heads_w = w_query.shape[1] // 2
    units = w_gate.shape[1] // 4
    padded = -(-units // LANES) * LANES

    piece, gathered = (2, units, depth), (2, padded, width)
    if depth % LANES:
        piece, gathered = (depth, 2 * padded), (width, 2 * padded)
    bf16 = jnp.bfloat16
    vmem = pl.BlockSpec(memory_space=pltpu.VMEM)
    blocks = pltpu.VMEM((3, count, rows, cols), bf16)
    share = pltpu.VMEM((rows, cols), bf16)
    chunk = rows // 2
    chunks = 2 * rows // chunk
    dma = pltpu.SemaphoreType.DMA
    return pl.pallas_call(
        functools.partial(layer_kernel, planes, chips),
        out_shape=jax.ShapeDtypeStruct((rows, cols), bf16),
        in_specs=[vmem] * 10,
        out_specs=vmem,
        scratch_shapes=[
            pltpu.VMEM((width, heads_w + HEAD_DIM), bf16),
            pltpu.VMEM((2 * planes, heads_w, depth), bf16),
            pltpu.VMEM((2, 2, *piece), bf16),
            pltpu.VMEM(gathered, bf16),
            pltpu.VMEM((2, *piece), bf16),
            pltpu.VMEM((2 * planes, padded, depth), bf16),
            pltpu.VMEM((2, units, depth), bf16),
            pltpu.VMEM((2 * rows, width), bf16),
            pltpu.VMEM((2, 2 * rows, width), bf16),
            pltpu.VMEM((2 * rows, width), bf16),
            pltpu.VMEM((2 * rows, heads_w), bf16),
            pltpu.VMEM((2, 4 * rows, HEAD_DIM), bf16),
            pltpu.VMEM((4 * rows, padded), bf16),
            pltpu.VMEM((2, count, rows, cols), bf16), blocks, blocks,
            pltpu.VMEM((3, count - 1, rows, cols), bf16),
            share, share,
            pltpu.VMEM((2, rows, cols), bf16),
            dma((3,)), dma((3,)),
            dma((2, planes, 2, 2)), dma((planes, 2, 2)),
            dma((2, 2)), dma((2, 2)),
            dma((planes, 2, 2)), dma((planes, 2, 2)),
            dma((5, 2)), dma((2, 2)),
            dma((3, count, 2)), dma((3, count, 2)), dma((3, count, 2)), dma((3, count, 2)),
            dma((3, chunks)), dma((3, chunks)),
            dma((2, 2)), dma((2, 2)),
            dma((3, count, 2)), dma((3, count, 2)), dma((3, count, 2)), dma((3, count, 2)),
        ],
        compiler_params=pltpu.CompilerParams(
            collective_id=1, has_side_effects=True, vmem_limit_bytes=66_900_000
        ),
    )(
        tokens, attn_gain.reshape(1, -1), mlp_gain.reshape(1, -1),
        w_query, w_key, w_value, w_out, w_gate, w_up, w_down,
    )


def solution(mesh):
    sizes = mesh.shape
    split = Mesh(
        mesh.devices.reshape(sizes["seq"] // 2, 2, sizes["tensor"]), ("hi", "pair", "tensor")
    )
    seq = ("hi", "pair")
    in_specs = (
        P(seq, "tensor"),
        P(),
        P(seq, "tensor"),
        P(seq, "tensor"),
        P(seq, "tensor"),
        P("tensor", seq),
        P(),
        P(seq, "tensor"),
        P(seq, "tensor"),
        P("tensor", seq),
    )
    return jax.shard_map(
        per_device, mesh=split, in_specs=in_specs, out_specs=P(seq, "tensor"), check_vma=False
    )
```
